32 devices in a mesh: dp: 8 (over y, x, core), mp: 4 (over z).
Axes of the slice: x: 2, y: 2, z: 4, core: 2. Of those that a mesh axis runs over, the one named last changes fastest.
Arguments:
- img_tokens: bfloat16 [32, 128, 1408], P(('dp', 'mp')), may hold values from -6 to 6
- w_key: bfloat16 [1408, 2048], P(None, 'mp'), may hold values from -0.15625 to 0.15625
- w_value: bfloat16 [1408, 2048], P(None, 'mp'), may hold values from -0.15625 to 0.15625
- queries: bfloat16 [32, 32, 2048], P('dp', None, 'mp'), may hold values from -6 to 6
- lengths: int32 [32], P('dp'), may hold values from 1 to 32
- d_out: bfloat16 [32, 32, 2048], P('dp', None, 'mp'), may hold values from -6 to 6
- img_pooled: bfloat16 [32, 1408], P(('dp', 'mp')), may hold values from -40 to 40
- w_proj: bfloat16 [1408, 2048], P(None, 'mp'), may hold values from -0.19921875 to 0.19921875
- txt_embed: bfloat16 [32, 2048], P('dp', 'mp'), may hold values from -80 to 80
- inv_temp: float32 [1], replicated, may hold values from 30 to 100
Outputs:
- attended: bfloat16 [32, 32, 2048], P('dp', None, 'mp')
- grad_queries: bfloat16 [32, 32, 2048], P('dp', None, 'mp')
- dw_key: float32 [1408, 2048], P('dp', 'mp')
- dw_value: float32 [1408, 2048], P('dp', 'mp')
- contrast: float32 [2, 32], P(None, 'dp')
The draws below stay inside these ranges and needn't reach their ends.
Inputs may be any that keep to these rules, and one draw needn't show every extreme that they name: lengths: each caption's count of real positions.
All inputs are finite; a program needn't handle non-finite values.
Results may differ from the reference program's by a relative error of at most 0.0081.
Values may be sent and summed in bfloat16 or wider, within the bound.
No kernel may reach another device: no remote copies, remote signals or barrier semaphores. Data moves between devices by JAX's collectives and lax.ppermute only.
A program may use at most 64 MiB of HBM per device.

```python
import math
import jax
import jax.numpy as jnp
from jax import lax

D = 2048
DI = 1408
HEADS = 16
HD = 128
NTOK = 128
LQ = 32
GROUP = 4
BATCH = 32


def joint_embeddings(key):
    subkeys = [jax.random.fold_in(key, 7001 + n) for n in range(10)]
    centers = jax.random.normal(subkeys[0], (16, DI), jnp.float32)
    strengths = jnp.exp(jax.random.uniform(subkeys[1], (16,), jnp.float32, math.log(0.3), 0.0))
    drawn = jax.random.randint(subkeys[2], (BATCH,), 0, 64)
    member = drawn * drawn // 256
    one_hot = (member[:, None] == jnp.arange(16)[None, :]).astype(jnp.float32)
    picked = jnp.dot(one_hot, centers * strengths[:, None])
    mixing = jax.random.uniform(subkeys[3], (BATCH, 1), jnp.float32, 0.15, 0.6)
    w_proj = jnp.clip(jax.random.normal(subkeys[4], (DI, D), jnp.float32) * DI ** (-0.5), -0.19921875, 0.19921875)
    noise_part = jax.random.normal(subkeys[5], (BATCH, DI), jnp.float32)
    pooled = jnp.clip(picked + noise_part, -8.0, 8.0)
    projected = jnp.dot(pooled, w_proj)
    direction = projected * jax.lax.rsqrt(jnp.sum(projected * projected, axis=1, keepdims=True) + 1e-06)
    aligned = mixing * math.sqrt(D) * direction
    text_noise = jax.random.normal(subkeys[8], (BATCH, D), jnp.float32)
    text = jnp.clip(aligned + text_noise, -8.0, 8.0)
    return (pooled, w_proj, text)


def draw_img_pooled(key, part):
    return joint_embeddings(key)[0].astype(jnp.bfloat16)


def draw_w_proj(key, part):
    return joint_embeddings(key)[1].astype(jnp.bfloat16)


def draw_txt_embed(key, part):
    return joint_embeddings(key)[2].astype(jnp.bfloat16)


def place_ends(result, rng, low, high):
    longest = result.shape.index(max(result.shape))
    spots = []
    for shift in (0, 1):
        where = [jax.random.randint(jax.random.fold_in(rng, axis), (), 0, length) for axis, length in enumerate(result.shape)]
        where[longest] = (where[longest] + shift) % result.shape[longest]
        spots.append(tuple(where))
    return result.at[spots[0]].set(low).at[spots[1]].set(high)


def shard_levels(stream_key, dims, cuts, smallest, largest):
    def one(axis_at, shards_of):
        draws = jax.random.uniform(jax.random.fold_in(jax.random.fold_in(stream_key, 6), axis_at), (shards_of,), jnp.float32, smallest / len(cuts), largest / len(cuts))
        return jnp.repeat(jnp.exp(draws), dims[axis_at] // shards_of).reshape((-1,) + (1,) * (len(dims) - axis_at - 1))

    level = one(*cuts[0])
    for cut in cuts[1:]:
        level = level * one(*cut)
    return level


def gaussian(own_key, dims, deviation, reach, pieces=(), kind=jnp.bfloat16):
    gain = shard_levels(own_key, dims, pieces, -0.22, 0.18) if pieces else 1.0
    entries = jax.random.normal(own_key, dims, jnp.float32) * deviation * gain
    return jnp.minimum(jnp.maximum(entries, -reach), reach).astype(kind)


def setup_inputs(seed: int = 0) -> dict:
    seeds = jax.random.split(jax.random.key(seed), 11)
    return {
        "img_tokens": gaussian(seeds[0], (BATCH, NTOK, DI), 1.0, 6.0, ((0, 32),)),
        "w_key": gaussian(seeds[1], (DI, D), DI ** -0.5, 0.15625, ((1, 4),)),
        "w_value": gaussian(seeds[2], (DI, D), DI ** -0.5, 0.15625, ((1, 4),)),
        "queries": gaussian(seeds[3], (BATCH, LQ, D), 1.0, 6.0, ((0, 8), (2, 4))),
        "lengths": place_ends(jax.random.randint(seeds[4], (BATCH,), 1, LQ + 1), jax.random.fold_in(seeds[4], 1), 1, LQ).astype(jnp.int32),
        "d_out": gaussian(seeds[5], (BATCH, LQ, D), 1.0, 6.0, ((0, 8), (2, 4))),
        "img_pooled": draw_img_pooled(jax.random.fold_in(seeds[10], 71), 0),
        "w_proj": draw_w_proj(jax.random.fold_in(seeds[10], 71), 0),
        "txt_embed": draw_txt_embed(jax.random.fold_in(seeds[10], 71), 0),
        "inv_temp": jnp.clip(jnp.exp(jax.random.uniform(seeds[9], (1,), jnp.float32, math.log(30.0), math.log(100.0))), 30.0, 100.0),
    }


def attend_block(tokens, queries, lengths, d_out, w_key, w_value):
    count = tokens.shape[0]
    flat = tokens.reshape(count * NTOK, DI)
    keys = jnp.dot(flat, w_key, preferred_element_type=jnp.float32).astype(jnp.bfloat16).reshape(count, NTOK, HEADS, HD)
    values = jnp.dot(flat, w_value, preferred_element_type=jnp.float32).astype(jnp.bfloat16).reshape(count, NTOK, HEADS, HD)
    query_heads = queries.reshape(count, LQ, HEADS, HD).astype(jnp.float32)
    inv_root = HD ** (-0.5)
    scores = jnp.einsum('blhd,bthd->bhlt', query_heads, keys.astype(jnp.float32)) * inv_root
    probs = jax.nn.softmax(scores, axis=-1)
    probs_b = probs.astype(jnp.bfloat16).astype(jnp.float32)
    keep_rows = (jnp.arange(LQ)[None, :] < lengths[:, None]).astype(jnp.float32)
    output = jnp.einsum('bhlt,bthd->blhd', probs_b, values.astype(jnp.float32)) * keep_rows[:, :, None, None]
    attended = output.reshape(count, LQ, D).astype(jnp.bfloat16)
    masked = (d_out.astype(jnp.float32) * keep_rows[:, :, None]).astype(jnp.bfloat16)
    grad_heads = masked.reshape(count, LQ, HEADS, HD).astype(jnp.float32)
    grad_values = jnp.einsum('bhlt,blhd->bthd', probs_b, grad_heads).astype(jnp.bfloat16)
    grad_probs = jnp.einsum('blhd,bthd->bhlt', grad_heads, values.astype(jnp.float32))
    row_dots = lax.optimization_barrier(jnp.sum(probs * grad_probs, axis=-1, keepdims=True))
    grad_scores = (probs * (grad_probs - row_dots) * inv_root).astype(jnp.bfloat16).astype(jnp.float32)
    grad_queries = jnp.einsum('bhlt,bthd->blhd', grad_scores, keys.astype(jnp.float32)).reshape(count, LQ, D).astype(jnp.bfloat16)
    grad_keys = jnp.einsum('bhlt,blhd->bthd', grad_scores, query_heads).astype(jnp.bfloat16)
    key_terms = jnp.dot(flat.T, grad_keys.reshape(count * NTOK, D), preferred_element_type=jnp.float32)
    value_terms = jnp.dot(flat.T, grad_values.reshape(count * NTOK, D), preferred_element_type=jnp.float32)
    return (attended, grad_queries, key_terms, value_terms)

def reference(img_tokens, w_key, w_value, queries, lengths, d_out, img_pooled, w_proj, txt_embed, inv_temp):
    blocks = BATCH // GROUP
    tok_blocks = img_tokens.reshape(blocks, GROUP, NTOK, DI)
    query_blocks = queries.reshape(blocks, GROUP, LQ, D)
    length_blocks = lengths.reshape(blocks, GROUP)
    grad_blocks = d_out.reshape(blocks, GROUP, LQ, D)

    def step(carry, inputs):
        attended, grad_queries, key_terms, value_terms = attend_block(inputs[0], inputs[1], inputs[2], inputs[3], w_key, w_value)
        return ((carry[0] + key_terms, carry[1] + value_terms), (attended, grad_queries))
    start = (jnp.zeros((DI, D), jnp.float32), jnp.zeros((DI, D), jnp.float32))
    sums, outputs = lax.scan(step, start, (tok_blocks, query_blocks, length_blocks, grad_blocks))
    attended = outputs[0].reshape(BATCH, LQ, D)
    grad_queries = outputs[1].reshape(BATCH, LQ, D)
    img_raw = jnp.dot(img_pooled, w_proj, preferred_element_type=jnp.float32).astype(jnp.bfloat16)
    img_sq = lax.optimization_barrier(jnp.sum(jnp.square(img_raw.astype(jnp.float32)), axis=1))
    txt_sq = lax.optimization_barrier(jnp.sum(jnp.square(txt_embed.astype(jnp.float32)), axis=1))
    dots = jnp.dot(img_raw, txt_embed.T, preferred_element_type=jnp.float32)
    logits = inv_temp[0] * dots * lax.rsqrt(img_sq + 1e-06)[:, None] * lax.rsqrt(txt_sq + 1e-06)[None, :]
    diagonal = jnp.diagonal(logits)
    image_side = jax.nn.logsumexp(logits, axis=1) - diagonal
    caption_side = jax.nn.logsumexp(logits, axis=0) - diagonal
    contrast = jnp.stack([image_side, caption_side])
    return (attended, grad_queries, sums[0], sums[1], contrast)
```

```python
import functools

import jax
import jax.numpy as jnp
from jax import lax
from jax.experimental import pallas as pl
from jax.experimental.pallas import tpu as pltpu
from jax.sharding import PartitionSpec as P

HD = 128
F32 = jnp.float32
BF16 = jnp.bfloat16


def dot(a, b, ca, cb):
    return lax.dot_general(a, b, (((ca,), (cb,)), ((), ())), preferred_element_type=F32)


def image_kernel(heads, idx, lens, tok, wk, wv, qs, dos, *rest):
    att, gq, tok_t, grads = rest[-4:]
    inv = HD ** (-0.5)
    width = heads * HD
    x = tok[0]
    keys = jnp.dot(x, wk[...], preferred_element_type=F32).astype(BF16)
    values = jnp.dot(x, wv[...], preferred_element_type=F32).astype(BF16)
    tok_t[...] = x.T
    q_all = qs[0]
    length = lens[idx[0]]
    keep = (lax.broadcasted_iota(jnp.int32, (q_all.shape[0], HD), 0) < length).astype(F32)
    cols = [slice(h * HD, (h + 1) * HD) for h in range(heads)]
    k = [keys[:, c] for c in cols]
    v = [values[:, c] for c in cols]
    q = [q_all[:, c] for c in cols]
    masked = [(dos[0, :, c].astype(F32) * keep).astype(BF16) for c in cols]
    scores = [dot(q[h], k[h], 1, 1) * inv for h in range(heads)]
    grad_probs = [dot(masked[h], v[h], 1, 1) for h in range(heads)]
    tops = [jnp.max(s, axis=1, keepdims=True) for s in scores]
    exps = [jnp.exp(s - t) for s, t in zip(scores, tops)]
    probs = [e / jnp.sum(e, axis=1, keepdims=True) for e in exps]
    probs_b = [p.astype(BF16) for p in probs]
    row_dots = [jnp.sum(p * g, axis=1, keepdims=True) for p, g in zip(probs, grad_probs)]
    grad_scores = [
        (p * (g - r) * inv).astype(BF16) for p, g, r in zip(probs, grad_probs, row_dots)
    ]
    for h, c in enumerate(cols):
        att[0, :, c] = (dot(probs_b[h], v[h], 1, 0) * keep).astype(BF16)
        gq[0, :, c] = dot(grad_scores[h], k[h], 1, 0).astype(BF16)
        grads[:, c] = dot(grad_scores[h], q[h], 0, 0).astype(BF16)
        grads[:, slice(width + h * HD, width + (h + 1) * HD)] = dot(
            probs_b[h], masked[h], 0, 0
        ).astype(BF16)


def image_step(slot, slots, index, lengths, tokens, w_key, w_value, queries, d_out, carried):
    captions, caption_len, width = queries.shape
    image_len, feats = tokens.shape[1:]
    whole = lambda i, a, b: (0, 0)
    here = lambda i, a, b: (a[0], 0, 0)
    block = pl.BlockSpec((1, caption_len, width), here)
    any_space = pl.BlockSpec(memory_space=pl.ANY)
    shapes = (
        jax.ShapeDtypeStruct(queries.shape, BF16),
        jax.ShapeDtypeStruct(queries.shape, BF16),
        jax.ShapeDtypeStruct((feats, slots * image_len), BF16),
        jax.ShapeDtypeStruct((slots * image_len, 2 * width), BF16),
    )
    aliases = {7 + n: n for n in range(4)} if carried else {}
    return pl.pallas_call(
        functools.partial(image_kernel, width // HD),
        grid_spec=pltpu.PrefetchScalarGridSpec(
            num_scalar_prefetch=2,
            grid=(1,),
            in_specs=[
                pl.BlockSpec((1, image_len, feats), lambda i, a, b: (0, 0, 0)),
                pl.BlockSpec((feats, width), whole),
                pl.BlockSpec((feats, width), whole),
                block,
                block,
            ]
            + [any_space] * len(carried),
            out_specs=[
                block,
                block,
                pl.BlockSpec((feats, image_len), lambda i, a, b: (0, slot)),
                pl.BlockSpec((image_len, 2 * width), lambda i, a, b: (slot, 0)),
            ],
        ),
        out_shape=shapes,
        input_output_aliases=aliases,
        compiler_params=pltpu.CompilerParams(vmem_limit_bytes=24 * 2**20),
        name="image_step",
    )(index, lengths, tokens, w_key, w_value, queries, d_out, *carried)


def terms_kernel(part, tok_t, grads, out):
    out[0] = jnp.dot(tok_t[0], grads[...], preferred_element_type=F32).astype(out.dtype)


def weight_terms(part, blocks, grads, dtype):
    n, rows, depth = blocks.shape
    width = grads.shape[1]
    return pl.pallas_call(
        terms_kernel,
        grid_spec=pltpu.PrefetchScalarGridSpec(
            num_scalar_prefetch=1,
            grid=(n // 2,),
            in_specs=[
                pl.BlockSpec((1, rows, depth), lambda i, p: (2 * i + p[0], 0, 0)),
                pl.BlockSpec((depth, width), lambda i, p: (0, 0)),
            ],
            out_specs=pl.BlockSpec((1, rows, width), lambda i, p: (i, 0, 0)),
        ),
        out_shape=jax.ShapeDtypeStruct((n // 2, rows, width), dtype),
        compiler_params=pltpu.CompilerParams(vmem_limit_bytes=24 * 2**20),
        name="weight_terms",
    )(part, blocks, grads)


def pair_kernel(order, kept, got, *outs):
    for m, out in enumerate(outs):
        place = order[m]
        out[...] = (kept[place] + got[place].astype(F32)).astype(out.dtype)


def pair_sums(order, kept, got):
    n, rows, width = kept.shape
    full = pl.BlockSpec(kept.shape, lambda i, o: (0, 0, 0))
    piece = pl.BlockSpec((rows, width), lambda i, o: (0, 0))
    return pl.pallas_call(
        pair_kernel,
        grid_spec=pltpu.PrefetchScalarGridSpec(
            num_scalar_prefetch=1, grid=(1,), in_specs=[full, full], out_specs=[piece] * n
        ),
        out_shape=[jax.ShapeDtypeStruct((rows, width), F32 if m == 0 else BF16) for m in range(n)],
        compiler_params=pltpu.CompilerParams(vmem_limit_bytes=24 * 2**20),
        name="pair_sums",
    )(order, kept, got)


def shift(array, axis, count, step):
    return lax.ppermute(array, axis, [(n, (n + step) % count) for n in range(count)])


def flip(array, axis, count, mask):
    return lax.ppermute(array, axis, [(n, n ^ mask) for n in range(count)])


def body(
    n_dp,
    n_mp,
    img_tokens,
    w_key,
    w_value,
    queries,
    lengths,
    d_out,
    img_pooled,
    w_proj,
    txt_embed,
    inv_temp,
):
    group = lax.axis_index("dp")
    place = lax.axis_index("mp")
    captions = queries.shape[0]
    width = queries.shape[2]
    feats = img_tokens.shape[2]

    steps = sorted(range(1, n_mp), key=lambda s: min(s, n_mp - s))
    arrived = [img_tokens] + [shift(img_tokens, "mp", n_mp, s) for s in steps]

    facts = jnp.concatenate([img_pooled, txt_embed.reshape(1, -1)], axis=1)
    mask = 1
    while mask < n_dp:
        facts = jnp.concatenate([facts, flip(facts, "dp", n_dp, mask)], axis=0)
        mask *= 2
    pooled = facts[:, :feats]
    texts = facts[:, feats:].reshape(n_dp * captions, width)

    carried = ()
    for slot, (step, tokens) in enumerate(zip([0] + steps, arrived)):
        index = ((place - step) % n_mp).astype(jnp.int32).reshape(1)
        carried = image_step(
            slot, n_mp, index, lengths, tokens, w_key, w_value, queries, d_out, carried
        )
    attended, grad_queries, tok_t, grads = carried

    blocks = tok_t.reshape(n_dp, feats // n_dp, tok_t.shape[1])
    core = (group % 2).astype(jnp.int32).reshape(1)
    sent = weight_terms(1 - core, blocks, grads, BF16)
    got = flip(sent, "dp", n_dp, 1)
    kept = weight_terms(core, blocks, grads, F32)
    half = n_dp // 2
    order = (group // 2 ^ jnp.arange(half)).astype(jnp.int32)
    pieces = pair_sums(order, kept, got)
    shares = pieces[0]
    for m in range(1, half):
        shares = shares + flip(pieces[m], "dp", n_dp, 2 * m).astype(F32)
    dw_key = shares[:, :width]
    dw_value = shares[:, width:]

    rows = [pooled] + [shift(pooled, "mp", n_mp, s) for s in range(1, n_mp)]
    turned = [rows[0]] + rows[:0:-1]
    stacked = jnp.concatenate(turned + turned, axis=0)
    start = ((n_mp - place) % n_mp) * n_dp
    ordered = lax.dynamic_slice_in_dim(stacked, start, n_mp * n_dp, 0)
    img_raw = jnp.dot(ordered, w_proj, preferred_element_type=F32).astype(BF16)
    dots = dot(img_raw, texts, 1, 1)
    img_sq = jnp.sum(jnp.square(img_raw.astype(F32)), axis=1, keepdims=True)
    txt_sq = jnp.sum(jnp.square(texts.astype(F32)), axis=1, keepdims=True)
    total = jnp.concatenate([dots, img_sq, txt_sq], axis=1)
    mask = 1
    while mask < n_mp:
        total = total + flip(total, "mp", n_mp, mask)
        mask *= 2
    count = n_dp * captions
    dots, img_sq, txt_sq = total[:, :count], total[:, count], total[:, count + 1]
    logits = (
        inv_temp[0]
        * dots
        * lax.rsqrt(img_sq + 1e-06)[:, None]
        * lax.rsqrt(txt_sq + 1e-06)[None, :]
    )
    mine = logits[::n_dp]
    diag = jnp.sum(mine[:, :captions] * jnp.eye(captions, dtype=F32), axis=1)
    image_side = jax.nn.logsumexp(mine, axis=1) - diag
    caption_side = jax.nn.logsumexp(logits[:, :captions], axis=0) - diag
    contrast = jnp.stack([image_side, caption_side])
    return (attended, grad_queries, dw_key, dw_value, contrast)


def solution(mesh):
    placed = (
        P(("dp", "mp"), None, None),
        P(None, "mp"),
        P(None, "mp"),
        P("dp", None, "mp"),
        P("dp"),
        P("dp", None, "mp"),
        P(("dp", "mp"), None),
        P(None, "mp"),
        P("dp", "mp"),
        P(),
    )
    return jax.shard_map(
        functools.partial(body, mesh.shape["dp"], mesh.shape["mp"]),
        mesh=mesh,
        in_specs=placed,
        out_specs=(
            P("dp", None, "mp"),
            P("dp", None, "mp"),
            P("dp", "mp"),
            P("dp", "mp"),
            P(None, "dp"),
        ),
        check_vma=False,
    )
```

```python
import functools

import jax
import jax.numpy as jnp
from jax import lax
from jax.experimental import pallas as pl
from jax.experimental.pallas import tpu as pltpu
from jax.sharding import PartitionSpec as P


HD = 128
F32 = jnp.float32
BF16 = jnp.bfloat16


def dot(a, b, ca, cb):
    return lax.dot_general(a, b, (((ca,), (cb,)), ((), ())), preferred_element_type=F32)


def pick(ready, choices, store):
    if len(choices) == 1:
        store[...] = choices[0][0]
        return

    @pl.when(ready == 1)
    def _():
        store[...] = choices[0][0]

    @pl.when(ready == 0)
    def _():
        store[...] = choices[1][0]


def group_kernel(heads, counts, flags, lens, *refs):
    n = len(counts)
    inputs, rest = refs[: sum(counts)], refs[sum(counts) :]
    wk, wv, qs, dos, att, gq, grads, kept, sent, store, turned = rest
    inv = HD ** (-0.5)
    width = heads * HD
    image_len = store.shape[0] // n
    core = flags[2 * n]
    spans = [slice(s * image_len, (s + 1) * image_len) for s in range(n)]
    at = 0
    for s, count in enumerate(counts):
        pick(flags[s], inputs[at : at + count], store.at[spans[s]])
        at += count
    x = store[...]
    keys = jnp.dot(x, wk[...], preferred_element_type=F32).astype(BF16)
    values = jnp.dot(x, wv[...], preferred_element_type=F32).astype(BF16)
    rows, half = turned.shape[1], turned.shape[0] // 2
    for s in range(n):
        flipped = x[spans[s]].T
        for m in range(2 * half):
            turned[m] = flipped[m * rows : (m + 1) * rows]
        for m in range(half):
            kept[s, m] = turned[2 * m + core]
            sent[s, m] = turned[2 * m + 1 - core]
    cols = [slice(h * HD, (h + 1) * HD) for h in range(heads)]
    pairs = [(s, c) for s in range(n) for c in cols]
    keep = []
    for s in range(n):
        length = lens[flags[n + s]]
        at_row = lax.broadcasted_iota(jnp.int32, (qs.shape[1], HD), 0)
        keep.append((at_row < length).astype(F32))
    k = [keys[spans[s], c] for s, c in pairs]
    v = [values[spans[s], c] for s, c in pairs]
    q = [qs[flags[n + s], :, c] for s, c in pairs]
    masked = [(dos[flags[n + s], :, c].astype(F32) * keep[s]).astype(BF16) for s, c in pairs]
    scores = [dot(a, b, 1, 1) * inv for a, b in zip(q, k)]
    grad_probs = [dot(a, b, 1, 1) for a, b in zip(masked, v)]
    tops = [jnp.max(s, axis=1, keepdims=True) for s in scores]
    exps = [jnp.exp(s - t) for s, t in zip(scores, tops)]
    probs = [e / jnp.sum(e, axis=1, keepdims=True) for e in exps]
    probs_b = [p.astype(BF16) for p in probs]
    row_dots = [jnp.sum(p * g, axis=1, keepdims=True) for p, g in zip(probs, grad_probs)]
    grad_scores = [
        (p * (g - r) * inv).astype(BF16) for p, g, r in zip(probs, grad_probs, row_dots)
    ]
    for i, (s, c) in enumerate(pairs):
        other = slice(width + c.start, width + c.stop)
        grads[spans[s], c] = dot(grad_scores[i], q[i], 0, 0).astype(BF16)
        grads[spans[s], other] = dot(probs_b[i], masked[i], 0, 0).astype(BF16)
        att[s, :, c] = (dot(probs_b[i], v[i], 1, 0) * keep[s]).astype(BF16)
        gq[s, :, c] = dot(grad_scores[i], k[i], 1, 0).astype(BF16)


def image_group(flags, lengths, choices, n_dp, w_key, w_value, queries, d_out):
    n = len(choices)
    caption_len, width = queries.shape[1:]
    image_len, feats = choices[0][0].shape[1:]
    rows, half = feats // n_dp, n_dp // 2
    flat = [c for several in choices for c in several]
    shapes = [
        (n, caption_len, width),
        (n, caption_len, width),
        (n * image_len, 2 * width),
        (n, half, rows, image_len),
        (n, half, rows, image_len),
    ]
    full = lambda shape: pl.BlockSpec(shape, lambda i, a, b: (0,) * len(shape))
    operands = [*flat, w_key, w_value, queries, d_out]
    return pl.pallas_call(
        functools.partial(group_kernel, width // HD, [len(c) for c in choices]),
        grid_spec=pltpu.PrefetchScalarGridSpec(
            num_scalar_prefetch=2,
            grid=(1,),
            in_specs=[full(o.shape) for o in operands],
            out_specs=[full(s) for s in shapes],
            scratch_shapes=[
                pltpu.VMEM((n * image_len, feats), BF16),
                pltpu.VMEM((n_dp, rows, image_len), BF16),
            ],
        ),
        out_shape=[jax.ShapeDtypeStruct(s, BF16) for s in shapes],
        compiler_params=pltpu.CompilerParams(vmem_limit_bytes=20 * 2**20),
        name="image_group",
    )(flags, lengths, *operands)


def terms_kernel(count, pieces, order, *refs):
    turned, grads, outs = refs[:count], refs[count : 2 * count], refs[2 * count :]
    right = jnp.concatenate([g[...] for g in grads], axis=0)
    for piece, out in zip(pieces, outs):
        place = order[piece]
        left = jnp.concatenate([t[s, place] for t in turned for s in range(t.shape[0])], axis=1)
        out[...] = jnp.dot(left, right, preferred_element_type=F32).astype(out.dtype)


def weight_terms(order, pieces, turned, grads):
    count = len(turned)
    rows, width = turned[0].shape[2], grads[0].shape[1]
    full = lambda shape: pl.BlockSpec(shape, lambda i, o: (0,) * len(shape))
    return pl.pallas_call(
        functools.partial(terms_kernel, count, pieces),
        grid_spec=pltpu.PrefetchScalarGridSpec(
            num_scalar_prefetch=1,
            grid=(1,),
            in_specs=[full(o.shape) for o in (*turned, *grads)],
            out_specs=[full((rows, width))] * len(pieces),
        ),
        out_shape=[
            jax.ShapeDtypeStruct((rows, width), F32 if piece == 0 else BF16) for piece in pieces
        ],
        compiler_params=pltpu.CompilerParams(vmem_limit_bytes=20 * 2**20),
        name="weight_terms",
    )(order, *turned, *grads)


def finish_kernel(*refs):
    own, arrived, outs = refs[0], refs[1:-2], refs[-2:]
    width = outs[0].shape[1]
    for side, out in enumerate(outs):
        cols = slice(side * width, (side + 1) * width)
        total = own[:, cols]
        for piece in arrived:
            total = total + piece[:, cols].astype(F32)
        out[...] = total


def finish(own, arrived):
    rows, width = own.shape
    shape = jax.ShapeDtypeStruct((rows, width // 2), F32)
    return pl.pallas_call(
        finish_kernel,
        out_shape=[shape, shape],
        compiler_params=pltpu.CompilerParams(vmem_limit_bytes=12 * 2**20),
        name="finish",
    )(own, *arrived)


def arrange_kernel(slots, place, *refs):
    count = len(slots)
    at = 0
    for g, several in enumerate(slots):
        for s in range(several):
            for side in range(2):
                refs[2 * count + side][place[at]] = refs[2 * g + side][s]
            at += 1


def arrange(images, parts, slots):
    shape = (sum(slots), *parts[0].shape[1:])
    full = lambda shape: pl.BlockSpec(shape, lambda i, o: (0,) * len(shape))
    return pl.pallas_call(
        functools.partial(arrange_kernel, slots),
        grid_spec=pltpu.PrefetchScalarGridSpec(
            num_scalar_prefetch=1,
            grid=(1,),
            in_specs=[full(p.shape) for p in parts],
            out_specs=[full(shape)] * 2,
        ),
        out_shape=[jax.ShapeDtypeStruct(shape, BF16)] * 2,
        compiler_params=pltpu.CompilerParams(vmem_limit_bytes=12 * 2**20),
        name="arrange",
    )(images, *parts)


def facts_kernel(pooled, texts, out):
    feats, width = pooled.shape[1], texts.shape[1]
    out[:, :feats] = pooled[...]
    for c in range(texts.shape[0]):
        out[:, feats + c * width : feats + (c + 1) * width] = texts[c : c + 1, :]


def join_facts(pooled, texts):
    return pl.pallas_call(
        facts_kernel,
        out_shape=jax.ShapeDtypeStruct((1, pooled.shape[1] + texts.size), BF16),
        compiler_params=pltpu.CompilerParams(vmem_limit_bytes=2 * 2**20),
        name="join_facts",
    )(pooled, texts)


def sims_kernel(place, *refs):
    facts, (w_proj, out, rows, texts) = refs[:-4], refs[-4:]
    n_dp = facts[0].shape[0]
    feats, width = w_proj.shape
    captions = texts.shape[0] // n_dp
    for r, piece in enumerate(facts):
        start = pl.multiple_of((place[0] ^ r) * n_dp, n_dp)
        rows[pl.ds(start, n_dp)] = piece[:, :feats].astype(F32)
    for c in range(captions):
        texts[c * n_dp : (c + 1) * n_dp] = facts[0][
            :, feats + c * width : feats + (c + 1) * width
        ].astype(F32)
    img_raw = jnp.dot(
        rows[...].astype(BF16), w_proj[...], preferred_element_type=F32
    ).astype(BF16)
    txt = texts[...]
    raw = img_raw.astype(F32)
    count = txt.shape[0]
    out[:, :count] = dot(img_raw, txt.astype(BF16), 1, 1)
    out[:, count : count + 1] = jnp.sum(raw * raw, axis=1, keepdims=True)
    out[:, count + 1 : count + 2] = jnp.sum(txt * txt, axis=1, keepdims=True)


def similarity_terms(place, facts, w_proj, captions):
    n_dp = facts[0].shape[0]
    count, feats = n_dp * len(facts), w_proj.shape[0]
    full = lambda shape: pl.BlockSpec(shape, lambda i, o: (0,) * len(shape))
    return pl.pallas_call(
        sims_kernel,
        grid_spec=pltpu.PrefetchScalarGridSpec(
            num_scalar_prefetch=1,
            grid=(1,),
            in_specs=[full(o.shape) for o in (*facts, w_proj)],
            out_specs=full((count, n_dp * captions + 2)),
            scratch_shapes=[
                pltpu.VMEM((count, feats), F32),
                pltpu.VMEM((n_dp * captions, w_proj.shape[1]), F32),
            ],
        ),
        out_shape=jax.ShapeDtypeStruct((count, n_dp * captions + 2), F32),
        compiler_params=pltpu.CompilerParams(vmem_limit_bytes=16 * 2**20),
        name="similarity_terms",
    )(place, *facts, w_proj)


def losses_kernel(n_dp, place, *refs):
    inv_temp, terms, (out, store) = refs[0], refs[1:-2], refs[-2:]
    for r, term in enumerate(terms):
        store[place[0] ^ r] = term[...]
    total = store[0]
    for r in range(1, len(terms)):
        total = total + store[r]
    count = total.shape[0]
    captions = out.shape[1]
    img_sq = total[:, count : count + 1]
    txt_sq = jnp.broadcast_to(total[:, count + 1 : count + 2], (count, HD)).T[0:1, :]
    scale = inv_temp[0]
    logits = scale * total[:, :count] * lax.rsqrt(img_sq + 1e-06) * lax.rsqrt(txt_sq + 1e-06)
    row_top = jnp.max(logits, axis=1, keepdims=True)
    row_lse = row_top + jnp.log(jnp.sum(jnp.exp(logits - row_top), axis=1, keepdims=True))
    col_top = jnp.max(logits, axis=0, keepdims=True)
    col_lse = col_top + jnp.log(jnp.sum(jnp.exp(logits - col_top), axis=0, keepdims=True))
    row = lax.broadcasted_iota(jnp.int32, (count, HD), 0)
    lane = lax.broadcasted_iota(jnp.int32, (count, HD), 1)
    mine = (row == lane * n_dp) & (lane < captions)
    grid_row = lax.broadcasted_iota(jnp.int32, (count, count), 0)
    grid_col = lax.broadcasted_iota(jnp.int32, (count, count), 1)
    diag = jnp.sum(jnp.where(grid_row == grid_col, logits, 0.0), axis=1, keepdims=True)
    image_side = jnp.sum(jnp.where(mine, row_lse - diag, 0.0), axis=0, keepdims=True)
    col_lse = jnp.sum(jnp.where(grid_row == grid_col, col_lse, 0.0), axis=1, keepdims=True)
    caption_side = jnp.sum(jnp.where(mine, col_lse - diag, 0.0), axis=0, keepdims=True)
    out[0:1, :] = image_side[:, :captions]
    out[1:2, :] = caption_side[:, :captions]


def large_losses(place, inv_temp, terms, n_dp):
    count = terms[0].shape[0]
    stacked = jnp.stack(terms)
    total = stacked[place[0] ^ 0]
    for z in range(1, len(terms)):
        total = total + stacked[place[0] ^ z]
    img_sq, txt_sq = total[:, count], total[:, count + 1]
    logits = (
        inv_temp[0]
        * total[:, :count]
        * lax.rsqrt(img_sq + 1e-06)[:, None]
        * lax.rsqrt(txt_sq + 1e-06)[None, :]
    )
    diag = jnp.diagonal(logits)[::n_dp]
    image_side = jax.nn.logsumexp(logits[::n_dp], axis=1) - diag
    caption_side = jax.nn.logsumexp(logits[:, ::n_dp], axis=0) - diag
    return jnp.stack([image_side, caption_side])


def losses(place, inv_temp, terms, n_dp, captions):
    shape = terms[0].shape
    if shape[0] > HD:
        return large_losses(place, inv_temp, terms, n_dp)
    full = lambda shape: pl.BlockSpec(shape, lambda i, o: (0,) * len(shape))
    return pl.pallas_call(
        functools.partial(losses_kernel, n_dp),
        grid_spec=pltpu.PrefetchScalarGridSpec(
            num_scalar_prefetch=1,
            grid=(1,),
            in_specs=[pl.BlockSpec(memory_space=pltpu.SMEM)] + [full(shape)] * len(terms),
            out_specs=full((2, captions)),
            scratch_shapes=[pltpu.VMEM((len(terms), *shape), F32)],
        ),
        out_shape=jax.ShapeDtypeStruct((2, captions), F32),
        compiler_params=pltpu.CompilerParams(vmem_limit_bytes=40 * 2**20),
        name="losses",
    )(place, inv_temp, *terms)


def flip(array, axis, count, mask):
    return lax.ppermute(array, axis, [(n, n ^ mask) for n in range(count)])


def body(n_dp, n_mp, *args):
    return work(n_dp, n_mp, *args)


def slot_groups(n_mp):
    return [[0], [1, n_mp - 1]] + [[s] for s in range(n_mp - 2, 1, -1)]


def work(
    n_dp,
    n_mp,
    img_tokens,
    w_key,
    w_value,
    queries,
    lengths,
    d_out,
    img_pooled,
    w_proj,
    txt_embed,
    inv_temp,
):
    group = lax.axis_index("dp").astype(jnp.int32)
    place = lax.axis_index("mp").astype(jnp.int32)
    captions = queries.shape[0]

    right, left = {0: img_tokens}, {0: img_tokens}
    for d in range(1, n_mp - 1):
        ups = [(n, n + 1) for n in range(d - 1, n_mp - 1)]
        downs = [(n_mp - 1 - a, n_mp - 1 - b) for a, b in ups]
        right[d] = lax.ppermute(right[d - 1], "mp", ups)
        left[d] = lax.ppermute(left[d - 1], "mp", downs)
        if d == 1:
            ends = [(0, n_mp - 1), (n_mp - 1, 0)]
            right[n_mp - 1] = left[n_mp - 1] = lax.ppermute(img_tokens, "mp", ends)

    facts = join_facts(img_pooled, txt_embed)
    mask = 1
    while mask < n_dp:
        facts = jnp.concatenate([facts, flip(facts, "dp", n_dp, mask)], axis=0)
        mask *= 2

    core = group % 2
    parts, turned, others, grads, other_grads, images = [], [], [], [], [], []
    groups = slot_groups(n_mp)
    for slots in groups:
        choices = [[right[s], left[n_mp - s]] if s else [img_tokens] for s in slots]
        here = [(place - s) % n_mp for s in slots]
        images += here
        flags = jnp.stack([(place >= s).astype(jnp.int32) for s in slots] + here + [core])
        att, gq, grad, kept, sent = image_group(
            flags, lengths, choices, n_dp, w_key, w_value, queries, d_out
        )
        parts += [att, gq]
        turned.append(kept)
        others.append(flip(sent, "dp", n_dp, 1))
        grads.append(grad)
        other_grads.append(flip(grad, "dp", n_dp, 1))

    half = n_dp // 2
    order = ((group // 2) ^ jnp.arange(half)).astype(jnp.int32)
    sides = (turned + others, grads + other_grads)
    (last,) = weight_terms(order, (half - 1,), *sides)
    arrived = [flip(last, "dp", n_dp, 2 * (half - 1))]
    pieces = weight_terms(order, tuple(range(half - 2, -1, -1)), *sides)
    for m, piece in zip(range(half - 2, 0, -1), pieces):
        arrived.append(flip(piece, "dp", n_dp, 2 * m))
    attended, grad_queries = arrange(jnp.stack(images), parts, [len(s) for s in groups])
    dw_key, dw_value = finish(pieces[-1], arrived)

    pools = [facts] + [flip(facts, "mp", n_mp, m) for m in range(1, n_mp)]
    spot = place.reshape(1)
    terms = similarity_terms(spot, pools, w_proj, captions)
    terms = [terms] + [flip(terms, "mp", n_mp, m) for m in range(1, n_mp)]
    contrast = losses(spot, inv_temp, terms, n_dp, captions)
    return (attended, grad_queries, dw_key, dw_value, contrast)


def solution(mesh):
    placed = (
        P(("dp", "mp"), None, None),
        P(None, "mp"),
        P(None, "mp"),
        P("dp", None, "mp"),
        P("dp"),
        P("dp", None, "mp"),
        P(("dp", "mp"), None),
        P(None, "mp"),
        P("dp", "mp"),
        P(),
    )
    n_dp, n_mp = mesh.shape["dp"], mesh.shape["mp"]
    return jax.shard_map(
        functools.partial(body, n_dp, n_mp),
        mesh=mesh,
        in_specs=placed,
        out_specs=(
            P("dp", None, "mp"),
            P("dp", None, "mp"),
            P("dp", "mp"),
            P("dp", "mp"),
            P(None, "dp"),
        ),
        check_vma=False,
    )
```

```python
import functools

import jax
import jax.numpy as jnp
from jax import lax
from jax.experimental import pallas as pl
from jax.experimental.pallas import tpu as pltpu
from jax.sharding import PartitionSpec as P


HD = 128
F32 = jnp.float32
BF16 = jnp.bfloat16


def dot(a, b, ca, cb):
    return lax.dot_general(a, b, (((ca,), (cb,)), ((), ())), preferred_element_type=F32)


def room(*arrays):
    total = sum(a.size * a.dtype.itemsize for a in arrays)
    return pltpu.CompilerParams(vmem_limit_bytes=min(2 * total + 3 * 2**20, 60 * 2**20))


def pick(flag, choices, store):
    if len(choices) == 1:
        store[...] = choices[0][0]
        return
    for number, choice in enumerate(choices):

        @pl.when(flag == number)
        def _(choice=choice):
            store[...] = choice[0]


def group_kernel(heads, counts, rules, ids, lens, *refs):
    n = len(counts)
    which = [rule[0](ids[1]) for rule in rules]
    image = [rule[1](ids[1]) for rule in rules]
    inputs, rest = refs[: sum(counts)], refs[sum(counts) + 1 :]
    wk, wv, qs, dos, att, gq, grads, kept, sent, store, turned = rest
    inv = HD ** (-0.5)
    width = heads * HD
    image_len = store.shape[0] // n
    core = ids[0] & 1
    spans = [slice(s * image_len, (s + 1) * image_len) for s in range(n)]
    at = 0
    for s, count in enumerate(counts):
        pick(which[s], inputs[at : at + count], store.at[spans[s]])
        at += count
    x = store[...]
    keys = jnp.dot(x, wk[...], preferred_element_type=F32).astype(BF16)
    values = jnp.dot(x, wv[...], preferred_element_type=F32).astype(BF16)
    rows, half = turned.shape[1], turned.shape[0] // 2
    for s in range(n):
        flipped = x[spans[s]].T
        for m in range(2 * half):
            turned[m] = flipped[m * rows : (m + 1) * rows]
        for m in range(half):
            kept[s, m] = turned[2 * m + core]
            sent[s, m] = turned[2 * m + 1 - core]
    cols = [slice(h * HD, (h + 1) * HD) for h in range(heads)]
    pairs = [(s, c) for s in range(n) for c in cols]
    keep = []
    for s in range(n):
        length = lens[image[s]]
        at_row = lax.broadcasted_iota(jnp.int32, (qs.shape[1], HD), 0)
        keep.append((at_row < length).astype(F32))
    k = [keys[spans[s], c] for s, c in pairs]
    v = [values[spans[s], c] for s, c in pairs]
    q = [qs[image[s], :, c] for s, c in pairs]
    masked = [(dos[image[s], :, c].astype(F32) * keep[s]).astype(BF16) for s, c in pairs]
    scores = [dot(a, b, 1, 1) * inv for a, b in zip(q, k)]
    grad_probs = [dot(a, b, 1, 1) for a, b in zip(masked, v)]
    tops = [jnp.max(s, axis=1, keepdims=True) for s in scores]
    exps = [jnp.exp(s - t) for s, t in zip(scores, tops)]
    probs = [e / jnp.sum(e, axis=1, keepdims=True) for e in exps]
    probs_b = [p.astype(BF16) for p in probs]
    row_dots = [jnp.sum(p * g, axis=1, keepdims=True) for p, g in zip(probs, grad_probs)]
    grad_scores = [
        (p * (g - r) * inv).astype(BF16) for p, g, r in zip(probs, grad_probs, row_dots)
    ]
    for i, (s, c) in enumerate(pairs):
        other = slice(width + c.start, width + c.stop)
        grads[spans[s], c] = dot(grad_scores[i], q[i], 0, 0).astype(BF16)
        grads[spans[s], other] = dot(probs_b[i], masked[i], 0, 0).astype(BF16)
        att[s, :, c] = (dot(probs_b[i], v[i], 1, 0) * keep[s]).astype(BF16)
        gq[s, :, c] = dot(grad_scores[i], k[i], 1, 0).astype(BF16)


def image_group(ids, lengths, members, n_dp, w_key, w_value, queries, d_out, first):
    choices, rules = [m[0] for m in members], [m[1:] for m in members]
    n = len(choices)
    caption_len, width = queries.shape[1:]
    image_len, feats = choices[0][0].shape[1:]
    rows, half = feats // n_dp, n_dp // 2
    flat = [c for several in choices for c in several]
    shapes = [
        (n, caption_len, width),
        (n, caption_len, width),
        (n * image_len, 2 * width),
        (n, half, rows, image_len),
        (n, half, rows, image_len),
    ]
    full = lambda shape: pl.BlockSpec(shape, lambda i, a, b: (0,) * len(shape))
    operands = [*flat, first, w_key, w_value, queries, d_out]
    results = [jax.ShapeDtypeStruct(s, BF16) for s in shapes]
    return pl.pallas_call(
        functools.partial(group_kernel, width // HD, [len(c) for c in choices], rules),
        grid_spec=pltpu.PrefetchScalarGridSpec(
            num_scalar_prefetch=2,
            grid=(1,),
            in_specs=[full(o.shape) for o in flat]
            + [pl.BlockSpec(memory_space=pl.ANY)]
            + [full(o.shape) for o in operands[-4:]],
            out_specs=[full(s) for s in shapes],
            scratch_shapes=[
                pltpu.VMEM((n * image_len, feats), BF16),
                pltpu.VMEM((n_dp, rows, image_len), BF16),
            ],
        ),
        out_shape=results,
        compiler_params=room(*operands, *results, operands[0]),
        name="image_group",
    )(ids, lengths, *operands)


def joined(turned, grads, place):
    left = jnp.concatenate([t[s, place] for t in turned for s in range(t.shape[0])], axis=1)
    return jnp.dot(left, jnp.concatenate([g[...] for g in grads]), preferred_element_type=F32)


def early_kernel(count, *refs):
    turned, grads, out = refs[:count], refs[count : 2 * count], refs[2 * count]
    for place in range(out.shape[0]):
        out[place] = joined(turned, grads, place)


def early_terms(turned, grads):
    half, rows = turned[0].shape[1:3]
    result = jax.ShapeDtypeStruct((half, rows, grads[0].shape[1]), F32)
    return pl.pallas_call(
        functools.partial(early_kernel, len(turned)),
        out_shape=result,
        compiler_params=room(*turned, *grads, result),
        name="early_terms",
    )(*turned, *grads)


def terms_kernel(count, pieces, ids, *refs):
    turned, grads, early = refs[:count], refs[count : 2 * count], refs[2 * count]
    for piece, out in zip(pieces, refs[2 * count + 1 :]):
        place = (ids[0] >> 1) ^ piece
        out[...] = (early[place] + joined(turned, grads, place)).astype(out.dtype)


def weight_terms(ids, pieces, turned, grads, early):
    count = len(turned)
    rows, width = early.shape[1:]
    full = lambda shape: pl.BlockSpec(shape, lambda i, o: (0,) * len(shape))
    one = pl.BlockSpec((1, rows, width), lambda i, o: ((o[0] >> 1) ^ pieces[0], 0, 0))
    results = [jax.ShapeDtypeStruct((rows, width), F32 if p == 0 else BF16) for p in pieces]
    if len(pieces) == 1:
        kernel = functools.partial(one_kernel, count, pieces[0])
    else:
        one, kernel = full(early.shape), functools.partial(terms_kernel, count, pieces)
    return pl.pallas_call(
        kernel,
        grid_spec=pltpu.PrefetchScalarGridSpec(
            num_scalar_prefetch=1,
            grid=(1,),
            in_specs=[full(o.shape) for o in (*turned, *grads)] + [one],
            out_specs=[full((rows, width))] * len(pieces),
        ),
        out_shape=results,
        compiler_params=room(*turned, *grads, *results, early),
        name="weight_terms",
    )(ids, *turned, *grads, early)


def one_kernel(count, piece, ids, *refs):
    turned, grads, early, out = refs[:count], refs[count : 2 * count], *refs[2 * count :]
    out[...] = (early[0] + joined(turned, grads, (ids[0] >> 1) ^ piece)).astype(out.dtype)


def finish_kernel(*refs):
    own, arrived, outs = refs[0], refs[1:-2], refs[-2:]
    width = outs[0].shape[1]
    for side, out in enumerate(outs):
        cols = slice(side * width, (side + 1) * width)
        total = own[:, cols]
        for piece in arrived:
            total = total + piece[:, cols].astype(F32)
        out[...] = total


def finish(own, arrived):
    rows, width = own.shape
    shape = jax.ShapeDtypeStruct((rows, width // 2), F32)
    return pl.pallas_call(
        finish_kernel,
        out_shape=[shape, shape],
        compiler_params=room(own, own, *arrived),
        name="finish",
    )(own, *arrived)


def arrange_kernel(slots, rules, ids, *refs):
    count = len(slots)
    at = 0
    for g, several in enumerate(slots):
        for s in range(several):
            for side in range(2):
                refs[2 * count + side][rules[at](ids[1])] = refs[2 * g + side][s]
            at += 1


def arrange(ids, rules, parts, slots):
    shape = (sum(slots), *parts[0].shape[1:])
    full = lambda shape: pl.BlockSpec(shape, lambda i, o: (0,) * len(shape))
    return pl.pallas_call(
        functools.partial(arrange_kernel, slots, rules),
        grid_spec=pltpu.PrefetchScalarGridSpec(
            num_scalar_prefetch=1,
            grid=(1,),
            in_specs=[full(p.shape) for p in parts],
            out_specs=[full(shape)] * 2,
        ),
        out_shape=[jax.ShapeDtypeStruct(shape, BF16)] * 2,
        compiler_params=room(*parts, *parts),
        name="arrange",
    )(ids, *parts)


def facts_kernel(pooled, texts, out):
    feats, width = pooled.shape[1], texts.shape[1]
    out[:, :feats] = pooled[...]
    for c in range(texts.shape[0]):
        out[:, feats + c * width : feats + (c + 1) * width] = texts[c : c + 1, :]


def tick_kernel(ids, out):
    out[...] = jnp.zeros_like(out) + ids[0]


def tick(ids):
    return pl.pallas_call(
        tick_kernel,
        grid_spec=pltpu.PrefetchScalarGridSpec(
            num_scalar_prefetch=1,
            grid=(1,),
            in_specs=[],
            out_specs=pl.BlockSpec((8, HD), lambda i, o: (0, 0)),
        ),
        out_shape=jax.ShapeDtypeStruct((8, HD), jnp.int32),
        cost_estimate=pl.CostEstimate(flops=10**9, bytes_accessed=24 * 2**20, transcendentals=0),
        compiler_params=pltpu.CompilerParams(vmem_limit_bytes=2**20),
        name="tick",
    )(ids)


def append_kernel(first, second, out, *pooled):
    rows = first.shape[0]
    out[:rows] = first[...]
    out[rows:] = second[...]
    for part in pooled:
        feats = part.shape[1]
        part[:rows] = first[:, :feats]
        part[rows:] = second[:, :feats]


def append(first, second, feats):
    rows, width = first.shape
    shapes = [(2 * rows, width)] + ([(2 * rows, feats)] if feats else [])
    return pl.pallas_call(
        append_kernel,
        out_shape=[jax.ShapeDtypeStruct(s, first.dtype) for s in shapes],
        compiler_params=room(first, second, first, second, first, second),
        name="append",
    )(first, second)


def join_facts(pooled, texts):
    return pl.pallas_call(
        facts_kernel,
        out_shape=jax.ShapeDtypeStruct((1, pooled.shape[1] + texts.size), BF16),
        compiler_params=pltpu.CompilerParams(vmem_limit_bytes=2 * 2**20),
        name="join_facts",
    )(pooled, texts)


def sims_kernel(ids, *refs):
    facts, (w_proj, out, rows, texts) = refs[:-4], refs[-4:]
    n_dp = facts[0].shape[0]
    feats, width = w_proj.shape
    captions = texts.shape[0] // n_dp
    for r, piece in enumerate(facts):
        start = pl.multiple_of((ids[1] ^ r) * n_dp, n_dp)
        rows[pl.ds(start, n_dp)] = piece[:, :feats].astype(F32)
    for c in range(captions):
        texts[c * n_dp : (c + 1) * n_dp] = facts[0][
            :, feats + c * width : feats + (c + 1) * width
        ].astype(F32)
    img_raw = jnp.dot(
        rows[...].astype(BF16), w_proj[...], preferred_element_type=F32
    ).astype(BF16)
    txt = texts[...]
    raw = img_raw.astype(F32)
    count = txt.shape[0]
    out[:, :count] = dot(img_raw, txt.astype(BF16), 1, 1)
    out[:, count : count + 1] = jnp.sum(raw * raw, axis=1, keepdims=True)
    out[:, count + 1 : count + 2] = jnp.sum(txt * txt, axis=1, keepdims=True)


def similarity_terms(ids, facts, w_proj, captions):
    n_dp = facts[0].shape[0]
    count, feats = n_dp * len(facts), w_proj.shape[0]
    full = lambda shape: pl.BlockSpec(shape, lambda i, o: (0,) * len(shape))
    return pl.pallas_call(
        sims_kernel,
        grid_spec=pltpu.PrefetchScalarGridSpec(
            num_scalar_prefetch=1,
            grid=(1,),
            in_specs=[full(o.shape) for o in (*facts, w_proj)],
            out_specs=full((count, n_dp * captions + 2)),
            scratch_shapes=[
                pltpu.VMEM((count, feats), F32),
                pltpu.VMEM((n_dp * captions, w_proj.shape[1]), F32),
            ],
        ),
        out_shape=jax.ShapeDtypeStruct((count, n_dp * captions + 2), F32),
        compiler_params=room(*facts, w_proj, facts[0], facts[0], facts[0]),
        name="similarity_terms",
    )(ids, *facts, w_proj)


def losses_kernel(n_dp, ids, *refs):
    inv_temp, terms, (out, store) = refs[0], refs[1:-2], refs[-2:]
    for r, term in enumerate(terms):
        store[ids[1] ^ r] = term[...]
    total = store[0]
    for r in range(1, len(terms)):
        total = total + store[r]
    count = total.shape[0]
    captions = out.shape[1]
    img_sq = total[:, count : count + 1]
    txt_sq = jnp.broadcast_to(total[:, count + 1 : count + 2], (count, HD)).T[0:1, :]
    scale = inv_temp[0]
    logits = scale * total[:, :count] * lax.rsqrt(img_sq + 1e-06) * lax.rsqrt(txt_sq + 1e-06)
    row_top = jnp.max(logits, axis=1, keepdims=True)
    row_lse = row_top + jnp.log(jnp.sum(jnp.exp(logits - row_top), axis=1, keepdims=True))
    col_top = jnp.max(logits, axis=0, keepdims=True)
    col_lse = col_top + jnp.log(jnp.sum(jnp.exp(logits - col_top), axis=0, keepdims=True))
    row = lax.broadcasted_iota(jnp.int32, (count, HD), 0)
    lane = lax.broadcasted_iota(jnp.int32, (count, HD), 1)
    mine = (row == lane * n_dp) & (lane < captions)
    grid_row = lax.broadcasted_iota(jnp.int32, (count, count), 0)
    grid_col = lax.broadcasted_iota(jnp.int32, (count, count), 1)
    diag = jnp.sum(jnp.where(grid_row == grid_col, logits, 0.0), axis=1, keepdims=True)
    image_side = jnp.sum(jnp.where(mine, row_lse - diag, 0.0), axis=0, keepdims=True)
    col_lse = jnp.sum(jnp.where(grid_row == grid_col, col_lse, 0.0), axis=1, keepdims=True)
    caption_side = jnp.sum(jnp.where(mine, col_lse - diag, 0.0), axis=0, keepdims=True)
    out[0:1, :] = image_side[:, :captions]
    out[1:2, :] = caption_side[:, :captions]


def large_losses(ids, inv_temp, terms, n_dp):
    count = terms[0].shape[0]
    stacked = jnp.stack(terms)
    total = stacked[ids[1]]
    for z in range(1, len(terms)):
        total = total + stacked[ids[1] ^ z]
    img_sq, txt_sq = total[:, count], total[:, count + 1]
    logits = (
        inv_temp[0]
        * total[:, :count]
        * lax.rsqrt(img_sq + 1e-06)[:, None]
        * lax.rsqrt(txt_sq + 1e-06)[None, :]
    )
    diag = jnp.diagonal(logits)[::n_dp]
    image_side = jax.nn.logsumexp(logits[::n_dp], axis=1) - diag
    caption_side = jax.nn.logsumexp(logits[:, ::n_dp], axis=0) - diag
    return jnp.stack([image_side, caption_side])


def losses(ids, inv_temp, terms, n_dp, captions):
    shape = terms[0].shape
    if shape[0] > HD:
        return large_losses(ids, inv_temp, terms, n_dp)
    full = lambda shape: pl.BlockSpec(shape, lambda i, o: (0,) * len(shape))
    return pl.pallas_call(
        functools.partial(losses_kernel, n_dp),
        grid_spec=pltpu.PrefetchScalarGridSpec(
            num_scalar_prefetch=1,
            grid=(1,),
            in_specs=[pl.BlockSpec(memory_space=pltpu.SMEM)] + [full(shape)] * len(terms),
            out_specs=full((2, captions)),
            scratch_shapes=[pltpu.VMEM((len(terms), *shape), F32)],
        ),
        out_shape=jax.ShapeDtypeStruct((2, captions), F32),
        compiler_params=room(*terms),
        name="losses",
    )(ids, inv_temp, *terms)


def flip(array, axis, count, mask):
    return lax.ppermute(array, axis, [(n, n ^ mask) for n in range(count)])


def body(n_dp, n_mp, *args):
    return work(n_dp, n_mp, *args)


def gather_images(tokens, n_mp):
    first = lambda z: 0
    own = ([tokens], first, lambda z: z)
    if n_mp != 4:
        rest = []
        for s in range(1, n_mp):
            pairs = [(n, (n + s) % n_mp) for n in range(n_mp)]
            rule = lambda z, s=s: lax.rem(z + (n_mp - s), n_mp)
            rest.append([([lax.ppermute(tokens, "mp", pairs)], first, rule)])
        return [[own], *rest]
    right = lax.ppermute(tokens, "mp", [(0, 1), (1, 2), (2, 3)])
    left = lax.ppermute(tokens, "mp", [(1, 0), (2, 1), (3, 2)])
    far = lax.ppermute(tokens, "mp", [(0, 3), (3, 0)])
    right_on = lax.ppermute(right, "mp", [(1, 2), (2, 3)])
    left_on = lax.ppermute(left, "mp", [(1, 0), (2, 1)])
    inner = lambda z: (z == 1) | (z == 2)
    near = ([left, right], lambda z: z & 1, lambda z: z ^ 1)
    other = (
        [far, left, right],
        lambda z: jnp.where(inner(z), z, 0),
        lambda z: z ^ 3,
    )
    last = ([left_on, right_on], lambda z: z >> 1, lambda z: z ^ 2)
    return [[own], [near], [other], [last]]


def work(
    n_dp,
    n_mp,
    img_tokens,
    w_key,
    w_value,
    queries,
    lengths,
    d_out,
    img_pooled,
    w_proj,
    txt_embed,
    inv_temp,
):
    ids = jnp.stack([lax.axis_index("dp"), lax.axis_index("mp")]).astype(jnp.int32)
    captions = queries.shape[0]

    groups = gather_images(img_tokens, n_mp)
    feats = img_pooled.shape[1]

    facts = join_facts(img_pooled, txt_embed)
    mask = 1
    while mask < n_dp:
        got = flip(facts, "dp", n_dp, mask)
        facts, *pooled = append(facts, got, feats if 2 * mask == n_dp else 0)
        mask *= 2

    first = tick(ids)
    parts, turned, others, grads, other_grads = [], [], [], [], []
    for members in groups:
        att, gq, grad, kept, sent = image_group(
            ids, lengths, members, n_dp, w_key, w_value, queries, d_out, first
        )
        parts += [att, gq]
        turned.append(kept)
        others.append(flip(sent, "dp", n_dp, 1))
        grads.append(grad)
        other_grads.append(flip(grad, "dp", n_dp, 1))

    half = n_dp // 2
    early = early_terms(turned[:-1] + others[:-1], grads[:-1] + other_grads[:-1])
    sides = (turned[-1:] + others[-1:], grads[-1:] + other_grads[-1:], early)
    (last,) = weight_terms(ids, (half - 1,), *sides)
    arrived = [flip(last, "dp", n_dp, 2 * (half - 1))]
    pieces = weight_terms(ids, tuple(range(half - 2, -1, -1)), *sides)
    for m, piece in zip(range(half - 2, 0, -1), pieces):
        arrived.append(flip(piece, "dp", n_dp, 2 * m))
    rules = [m[2] for members in groups for m in members]
    attended, grad_queries = arrange(ids, rules, parts, [len(m) for m in groups])
    dw_key, dw_value = finish(pieces[-1], arrived)

    (pooled,) = pooled
    pools = [facts] + [flip(pooled, "mp", n_mp, m) for m in range(1, n_mp)]
    terms = similarity_terms(ids, pools, w_proj, captions)
    terms = [terms] + [flip(terms, "mp", n_mp, m) for m in range(1, n_mp)]
    contrast = losses(ids, inv_temp, terms, n_dp, captions)
    return (attended, grad_queries, dw_key, dw_value, contrast)


def solution(mesh):
    placed = (
        P(("dp", "mp"), None, None),
        P(None, "mp"),
        P(None, "mp"),
        P("dp", None, "mp"),
        P("dp"),
        P("dp", None, "mp"),
        P(("dp", "mp"), None),
        P(None, "mp"),
        P("dp", "mp"),
        P(),
    )
    n_dp, n_mp = mesh.shape["dp"], mesh.shape["mp"]
    return jax.shard_map(
        functools.partial(body, n_dp, n_mp),
        mesh=mesh,
        in_specs=placed,
        out_specs=(
            P("dp", None, "mp"),
            P("dp", None, "mp"),
            P("dp", "mp"),
            P("dp", "mp"),
            P(None, "dp"),
        ),
        check_vma=False,
    )
```

```python
import functools

import jax
import jax.numpy as jnp
from jax import lax
from jax.experimental import pallas as pl
from jax.experimental.pallas import tpu as pltpu
from jax.sharding import PartitionSpec as P


HD = 128
F32 = jnp.float32
BF16 = jnp.bfloat16


def dot(a, b, ca, cb):
    return lax.dot_general(a, b, (((ca,), (cb,)), ((), ())), preferred_element_type=F32)


def room(*arrays):
    total = sum(a.size * a.dtype.itemsize for a in arrays)
    return pltpu.CompilerParams(vmem_limit_bytes=min(2 * total + 3 * 2**20, 60 * 2**20))


def pick(flag, choices, store):
    if len(choices) == 1:
        store[...] = choices[0][0]
        return
    for number, choice in enumerate(choices):

        @pl.when(flag == number)
        def _(choice=choice):
            store[...] = choice[0]


def group_kernel(heads, counts, rules, ids, lens, *refs):
    n = len(counts)
    which = [rule[0](ids[1]) for rule in rules]
    image = [rule[1](ids[1]) for rule in rules]
    inputs, rest = refs[: sum(counts)], refs[sum(counts) + 1 :]
    wk, wv, qs, dos, att, gq, grads, kept, sent, store, turned = rest
    inv = HD ** (-0.5)
    width = heads * HD
    image_len = store.shape[0] // n
    core = ids[0] & 1
    spans = [slice(s * image_len, (s + 1) * image_len) for s in range(n)]
    at = 0
    for s, count in enumerate(counts):
        pick(which[s], inputs[at : at + count], store.at[spans[s]])
        at += count
    x = store[...]
    keys = jnp.dot(x, wk[...], preferred_element_type=F32).astype(BF16)
    values = jnp.dot(x, wv[...], preferred_element_type=F32).astype(BF16)
    rows, half = turned.shape[1], turned.shape[0] // 2
    for s in range(n):
        flipped = x[spans[s]].T
        for m in range(2 * half):
            turned[m] = flipped[m * rows : (m + 1) * rows]
        for m in range(half):
            kept[s, m] = turned[2 * m + core]
            sent[s, m] = turned[2 * m + 1 - core]
    cols = [slice(h * HD, (h + 1) * HD) for h in range(heads)]
    pairs = [(s, c) for s in range(n) for c in cols]
    keep = []
    for s in range(n):
        length = lens[image[s]]
        at_row = lax.broadcasted_iota(jnp.int32, (qs.shape[1], HD), 0)
        keep.append((at_row < length).astype(F32))
    k = [keys[spans[s], c] for s, c in pairs]
    v = [values[spans[s], c] for s, c in pairs]
    q = [qs[image[s], :, c] for s, c in pairs]
    masked = [(dos[image[s], :, c].astype(F32) * keep[s]).astype(BF16) for s, c in pairs]
    scores = [dot(a, b, 1, 1) * inv for a, b in zip(q, k)]
    grad_probs = [dot(a, b, 1, 1) for a, b in zip(masked, v)]
    tops = [jnp.max(s, axis=1, keepdims=True) for s in scores]
    exps = [jnp.exp(s - t) for s, t in zip(scores, tops)]
    probs = [e / jnp.sum(e, axis=1, keepdims=True) for e in exps]
    probs_b = [p.astype(BF16) for p in probs]
    row_dots = [jnp.sum(p * g, axis=1, keepdims=True) for p, g in zip(probs, grad_probs)]
    grad_scores = [
        (p * (g - r) * inv).astype(BF16) for p, g, r in zip(probs, grad_probs, row_dots)
    ]
    for i, (s, c) in enumerate(pairs):
        other = slice(width + c.start, width + c.stop)
        grads[spans[s], c] = dot(grad_scores[i], q[i], 0, 0).astype(BF16)
        grads[spans[s], other] = dot(probs_b[i], masked[i], 0, 0).astype(BF16)
        att[s, :, c] = (dot(probs_b[i], v[i], 1, 0) * keep[s]).astype(BF16)
        gq[s, :, c] = dot(grad_scores[i], k[i], 1, 0).astype(BF16)


def image_group(ids, lengths, members, n_dp, w_key, w_value, queries, d_out, first):
    choices, rules = [m[0] for m in members], [m[1:] for m in members]
    n = len(choices)
    caption_len, width = queries.shape[1:]
    image_len, feats = choices[0][0].shape[1:]
    rows, half = feats // n_dp, n_dp // 2
    flat = [c for several in choices for c in several]
    shapes = [
        (n, caption_len, width),
        (n, caption_len, width),
        (n * image_len, 2 * width),
        (n, half, rows, image_len),
        (n, half, rows, image_len),
    ]
    full = lambda shape: pl.BlockSpec(shape, lambda i, a, b: (0,) * len(shape))
    operands = [*flat, first, w_key, w_value, queries, d_out]
    results = [jax.ShapeDtypeStruct(s, BF16) for s in shapes]
    return pl.pallas_call(
        functools.partial(group_kernel, width // HD, [len(c) for c in choices], rules),
        grid_spec=pltpu.PrefetchScalarGridSpec(
            num_scalar_prefetch=2,
            grid=(1,),
            in_specs=[full(o.shape) for o in flat]
            + [pl.BlockSpec(memory_space=pl.ANY)]
            + [full(o.shape) for o in operands[-4:]],
            out_specs=[full(s) for s in shapes],
            scratch_shapes=[
                pltpu.VMEM((n * image_len, feats), BF16),
                pltpu.VMEM((n_dp, rows, image_len), BF16),
            ],
        ),
        out_shape=results,
        compiler_params=room(*operands, *results, operands[0]),
    )(ids, lengths, *operands)


def joined(turned, grads, place):
    left = jnp.concatenate([t[s, place] for t in turned for s in range(t.shape[0])], axis=1)
    return jnp.dot(left, jnp.concatenate([g[...] for g in grads]), preferred_element_type=F32)


def early_kernel(count, *refs):
    turned, grads, out = refs[:count], refs[count : 2 * count], refs[2 * count]
    for place in range(out.shape[0]):
        out[place] = joined(turned, grads, place)


def early_terms(turned, grads):
    half, rows = turned[0].shape[1:3]
    result = jax.ShapeDtypeStruct((half, rows, grads[0].shape[1]), F32)
    return pl.pallas_call(
        functools.partial(early_kernel, len(turned)),
        out_shape=result,
        compiler_params=room(*turned, *grads, result),
    )(*turned, *grads)


def terms_kernel(count, pieces, ids, *refs):
    turned, grads, early = refs[:count], refs[count : 2 * count], refs[2 * count]
    for piece, out in zip(pieces, refs[2 * count + 1 :]):
        place = (ids[0] >> 1) ^ piece
        out[...] = (early[place] + joined(turned, grads, place)).astype(out.dtype)


def weight_terms(ids, pieces, turned, grads, early):
    count = len(turned)
    rows, width = early.shape[1:]
    full = lambda shape: pl.BlockSpec(shape, lambda i, o: (0,) * len(shape))
    one = pl.BlockSpec((1, rows, width), lambda i, o: ((o[0] >> 1) ^ pieces[0], 0, 0))
    results = [jax.ShapeDtypeStruct((rows, width), F32 if p == 0 else BF16) for p in pieces]
    if len(pieces) == 1:
        kernel = functools.partial(one_kernel, count, pieces[0])
    else:
        one, kernel = full(early.shape), functools.partial(terms_kernel, count, pieces)
    return pl.pallas_call(
        kernel,
        grid_spec=pltpu.PrefetchScalarGridSpec(
            num_scalar_prefetch=1,
            grid=(1,),
            in_specs=[full(o.shape) for o in (*turned, *grads)] + [one],
            out_specs=[full((rows, width))] * len(pieces),
        ),
        out_shape=results,
        compiler_params=room(*turned, *grads, *results, early),
    )(ids, *turned, *grads, early)


def one_kernel(count, piece, ids, *refs):
    turned, grads, early, out = refs[:count], refs[count : 2 * count], *refs[2 * count :]
    out[...] = (early[0] + joined(turned, grads, (ids[0] >> 1) ^ piece)).astype(out.dtype)


def part_kernel(count, wanted, ids, *refs):
    turned, grads, early = refs[:count], refs[count : 2 * count], refs[2 * count]
    outs = refs[2 * count + 1 :]
    width = early.shape[2] // 2
    for side in range(2):
        cols = slice(side * width, (side + 1) * width)
        needs = [(o, i, m) for o, w in enumerate(wanted) for i, (m, h) in enumerate(w) if h == side]
        if not needs:
            continue
        right = jnp.concatenate([g[:, cols] for g in grads])
        for o, i, m in needs:
            place = (ids[0] >> 1) ^ m
            left = jnp.concatenate(
                [t[n, place] for t in turned for n in range(t.shape[0])], axis=1
            )
            total = early[place, :, cols] + jnp.dot(left, right, preferred_element_type=F32)
            outs[o][i] = total.astype(outs[o].dtype)


def term_parts(ids, wanted, dtype, turned, grads, early):
    rows, width = early.shape[1], early.shape[2] // 2
    full = lambda shape: pl.BlockSpec(shape, lambda i, o: (0,) * len(shape))
    operands = [*turned, *grads, early]
    results = [jax.ShapeDtypeStruct((len(w), rows, width), dtype) for w in wanted]
    return pl.pallas_call(
        functools.partial(part_kernel, len(turned), wanted),
        grid_spec=pltpu.PrefetchScalarGridSpec(
            num_scalar_prefetch=1,
            grid=(1,),
            in_specs=[full(o.shape) for o in operands],
            out_specs=[full(r.shape) for r in results],
        ),
        out_shape=results,
        compiler_params=room(*operands, *results),
    )(ids, *operands)


def pass_kernel(side, kept, got, out):
    out[...] = (kept[side] + got[1].astype(F32)).astype(out.dtype)


def pass_on(side, kept, got):
    return pl.pallas_call(
        functools.partial(pass_kernel, side),
        out_shape=jax.ShapeDtypeStruct(kept.shape[1:], BF16),
        compiler_params=room(kept, got, got),
    )(kept, got)


def half_finish_kernel(side, own, first, second, out):
    out[...] = own[side] + first[0].astype(F32) + second[...].astype(F32)


def half_finish(side, own, first, second):
    return pl.pallas_call(
        functools.partial(half_finish_kernel, side),
        out_shape=jax.ShapeDtypeStruct(own.shape[1:], F32),
        compiler_params=room(own, first, second),
    )(own, first, second)


def direct_sums(ids, n_dp, sides):
    half = n_dp // 2
    (last,) = weight_terms(ids, (half - 1,), *sides)
    arrived = [flip(last, "dp", n_dp, 2 * (half - 1))]
    pieces = weight_terms(ids, tuple(range(half - 2, -1, -1)), *sides)
    for m, piece in zip(range(half - 2, 0, -1), pieces):
        arrived.append(flip(piece, "dp", n_dp, 2 * m))
    return finish(pieces[-1], arrived)


def staged_sums(ids, n_dp, sides):
    key_send, value_send = term_parts(ids, [[(1, 0), (3, 0)], [(2, 1), (3, 1)]], BF16, *sides)
    key_1 = flip(key_send, "dp", n_dp, 2)
    value_1 = flip(value_send, "dp", n_dp, 4)
    own, kept = term_parts(ids, [[(0, 0), (0, 1)], [(2, 0), (1, 1)]], F32, *sides)
    key_on = pass_on(0, kept, key_1)
    key_2 = flip(key_on, "dp", n_dp, 4)
    value_on = pass_on(1, kept, value_1)
    value_2 = flip(value_on, "dp", n_dp, 2)
    dw_key = half_finish(0, own, key_1, key_2)
    return dw_key, half_finish(1, own, value_1, value_2)


def finish_kernel(*refs):
    own, arrived, outs = refs[0], refs[1:-2], refs[-2:]
    width = outs[0].shape[1]
    for side, out in enumerate(outs):
        cols = slice(side * width, (side + 1) * width)
        total = own[:, cols]
        for piece in arrived:
            total = total + piece[:, cols].astype(F32)
        out[...] = total


def finish(own, arrived):
    rows, width = own.shape
    shape = jax.ShapeDtypeStruct((rows, width // 2), F32)
    return pl.pallas_call(
        finish_kernel,
        out_shape=[shape, shape],
        compiler_params=room(own, own, *arrived),
    )(own, *arrived)


def arrange_kernel(slots, rules, ids, *refs):
    count = len(slots)
    at = 0
    for g, several in enumerate(slots):
        for s in range(several):
            for side in range(2):
                refs[2 * count + side][rules[at](ids[1])] = refs[2 * g + side][s]
            at += 1


def arrange(ids, rules, parts, slots):
    shape = (sum(slots), *parts[0].shape[1:])
    full = lambda shape: pl.BlockSpec(shape, lambda i, o: (0,) * len(shape))
    return pl.pallas_call(
        functools.partial(arrange_kernel, slots, rules),
        grid_spec=pltpu.PrefetchScalarGridSpec(
            num_scalar_prefetch=1,
            grid=(1,),
            in_specs=[full(p.shape) for p in parts],
            out_specs=[full(shape)] * 2,
        ),
        out_shape=[jax.ShapeDtypeStruct(shape, BF16)] * 2,
        compiler_params=room(*parts, *parts),
    )(ids, *parts)


def facts_kernel(pooled, texts, out):
    feats, width = pooled.shape[1], texts.shape[1]
    out[:, :feats] = pooled[...]
    for c in range(texts.shape[0]):
        out[:, feats + c * width : feats + (c + 1) * width] = texts[c : c + 1, :]


def tick_kernel(ids, out):
    out[...] = jnp.zeros_like(out) + ids[0]


def tick(ids):
    return pl.pallas_call(
        tick_kernel,
        grid_spec=pltpu.PrefetchScalarGridSpec(
            num_scalar_prefetch=1,
            grid=(1,),
            in_specs=[],
            out_specs=pl.BlockSpec((8, HD), lambda i, o: (0, 0)),
        ),
        out_shape=jax.ShapeDtypeStruct((8, HD), jnp.int32),
        cost_estimate=pl.CostEstimate(flops=10**9, bytes_accessed=24 * 2**20, transcendentals=0),
        compiler_params=pltpu.CompilerParams(vmem_limit_bytes=2**20),
    )(ids)


def append_kernel(first, second, out, *pooled):
    rows = first.shape[0]
    out[:rows] = first[...]
    out[rows:] = second[...]
    for part in pooled:
        feats = part.shape[1]
        part[:rows] = first[:, :feats]
        part[rows:] = second[:, :feats]


def append(first, second, feats):
    rows, width = first.shape
    shapes = [(2 * rows, width)] + ([(2 * rows, feats)] if feats else [])
    return pl.pallas_call(
        append_kernel,
        out_shape=[jax.ShapeDtypeStruct(s, first.dtype) for s in shapes],
        compiler_params=room(first, second, first, second, first, second),
    )(first, second)


def join_facts(pooled, texts):
    return pl.pallas_call(
        facts_kernel,
        out_shape=jax.ShapeDtypeStruct((1, pooled.shape[1] + texts.size), BF16),
        compiler_params=pltpu.CompilerParams(vmem_limit_bytes=2 * 2**20),
    )(pooled, texts)


def sims_kernel(ids, *refs):
    facts, (w_proj, out, rows, texts) = refs[:-4], refs[-4:]
    n_dp = facts[0].shape[0]
    feats, width = w_proj.shape
    captions = texts.shape[0] // n_dp
    for r, piece in enumerate(facts):
        start = pl.multiple_of((ids[1] ^ r) * n_dp, n_dp)
        rows[pl.ds(start, n_dp)] = piece[:, :feats].astype(F32)
    for c in range(captions):
        texts[c * n_dp : (c + 1) * n_dp] = facts[0][
            :, feats + c * width : feats + (c + 1) * width
        ].astype(F32)
    img_raw = jnp.dot(
        rows[...].astype(BF16), w_proj[...], preferred_element_type=F32
    ).astype(BF16)
    txt = texts[...]
    raw = img_raw.astype(F32)
    count = txt.shape[0]
    out[:, :count] = dot(img_raw, txt.astype(BF16), 1, 1)
    out[:, count : count + 1] = jnp.sum(raw * raw, axis=1, keepdims=True)
    out[:, count + 1 : count + 2] = jnp.sum(txt * txt, axis=1, keepdims=True)


def similarity_terms(ids, facts, w_proj, captions):
    n_dp = facts[0].shape[0]
    count, feats = n_dp * len(facts), w_proj.shape[0]
    full = lambda shape: pl.BlockSpec(shape, lambda i, o: (0,) * len(shape))
    return pl.pallas_call(
        sims_kernel,
        grid_spec=pltpu.PrefetchScalarGridSpec(
            num_scalar_prefetch=1,
            grid=(1,),
            in_specs=[full(o.shape) for o in (*facts, w_proj)],
            out_specs=full((count, n_dp * captions + 2)),
            scratch_shapes=[
                pltpu.VMEM((count, feats), F32),
                pltpu.VMEM((n_dp * captions, w_proj.shape[1]), F32),
            ],
        ),
        out_shape=jax.ShapeDtypeStruct((count, n_dp * captions + 2), F32),
        compiler_params=room(*facts, w_proj, facts[0], facts[0], facts[0]),
    )(ids, *facts, w_proj)


def losses_kernel(n_dp, ids, *refs):
    inv_temp, terms, (out, store) = refs[0], refs[1:-2], refs[-2:]
    for r, term in enumerate(terms):
        store[ids[1] ^ r] = term[...]
    total = store[0]
    for r in range(1, len(terms)):
        total = total + store[r]
    count = total.shape[0]
    captions = out.shape[1]
    img_sq = total[:, count : count + 1]
    txt_sq = jnp.broadcast_to(total[:, count + 1 : count + 2], (count, HD)).T[0:1, :]
    scale = inv_temp[0]
    logits = scale * total[:, :count] * lax.rsqrt(img_sq + 1e-06) * lax.rsqrt(txt_sq + 1e-06)
    row_top = jnp.max(logits, axis=1, keepdims=True)
    row_lse = row_top + jnp.log(jnp.sum(jnp.exp(logits - row_top), axis=1, keepdims=True))
    col_top = jnp.max(logits, axis=0, keepdims=True)
    col_lse = col_top + jnp.log(jnp.sum(jnp.exp(logits - col_top), axis=0, keepdims=True))
    row = lax.broadcasted_iota(jnp.int32, (count, HD), 0)
    lane = lax.broadcasted_iota(jnp.int32, (count, HD), 1)
    mine = (row == lane * n_dp) & (lane < captions)
    grid_row = lax.broadcasted_iota(jnp.int32, (count, count), 0)
    grid_col = lax.broadcasted_iota(jnp.int32, (count, count), 1)
    diag = jnp.sum(jnp.where(grid_row == grid_col, logits, 0.0), axis=1, keepdims=True)
    image_side = jnp.sum(jnp.where(mine, row_lse - diag, 0.0), axis=0, keepdims=True)
    col_lse = jnp.sum(jnp.where(grid_row == grid_col, col_lse, 0.0), axis=1, keepdims=True)
    caption_side = jnp.sum(jnp.where(mine, col_lse - diag, 0.0), axis=0, keepdims=True)
    out[0:1, :] = image_side[:, :captions]
    out[1:2, :] = caption_side[:, :captions]


def large_losses(ids, inv_temp, terms, n_dp):
    count = terms[0].shape[0]
    stacked = jnp.stack(terms)
    total = stacked[ids[1]]
    for z in range(1, len(terms)):
        total = total + stacked[ids[1] ^ z]
    img_sq, txt_sq = total[:, count], total[:, count + 1]
    logits = (
        inv_temp[0]
        * total[:, :count]
        * lax.rsqrt(img_sq + 1e-06)[:, None]
        * lax.rsqrt(txt_sq + 1e-06)[None, :]
    )
    diag = jnp.diagonal(logits)[::n_dp]
    image_side = jax.nn.logsumexp(logits[::n_dp], axis=1) - diag
    caption_side = jax.nn.logsumexp(logits[:, ::n_dp], axis=0) - diag
    return jnp.stack([image_side, caption_side])


def losses(ids, inv_temp, terms, n_dp, captions):
    shape = terms[0].shape
    if shape[0] > HD:
        return large_losses(ids, inv_temp, terms, n_dp)
    full = lambda shape: pl.BlockSpec(shape, lambda i, o: (0,) * len(shape))
    return pl.pallas_call(
        functools.partial(losses_kernel, n_dp),
        grid_spec=pltpu.PrefetchScalarGridSpec(
            num_scalar_prefetch=1,
            grid=(1,),
            in_specs=[pl.BlockSpec(memory_space=pltpu.SMEM)] + [full(shape)] * len(terms),
            out_specs=full((2, captions)),
            scratch_shapes=[pltpu.VMEM((len(terms), *shape), F32)],
        ),
        out_shape=jax.ShapeDtypeStruct((2, captions), F32),
        compiler_params=room(*terms),
    )(ids, inv_temp, *terms)


def flip(array, axis, count, mask):
    return lax.ppermute(array, axis, [(n, n ^ mask) for n in range(count)])


def body(n_dp, n_mp, *args):
    return work(n_dp, n_mp, *args)


def gather_images(tokens, n_mp):
    first = lambda z: 0
    own = ([tokens], first, lambda z: z)
    if n_mp != 4:
        rest = []
        for s in range(1, n_mp):
            pairs = [(n, (n + s) % n_mp) for n in range(n_mp)]
            rule = lambda z, s=s: lax.rem(z + (n_mp - s), n_mp)
            rest.append([([lax.ppermute(tokens, "mp", pairs)], first, rule)])
        return [[own], *rest]
    inner = lambda z: ((z == 1) | (z == 2)).astype(jnp.int32)
    near = flip(tokens, "mp", n_mp, 1)
    cross = lax.ppermute(tokens, "mp", [(1, 2), (2, 1)])
    far = lax.ppermute(tokens, "mp", [(0, 3), (3, 0)])
    cross_on = lax.ppermute(cross, "mp", [(2, 3), (1, 0)])
    near_on = lax.ppermute(near, "mp", [(1, 2), (2, 1)])
    return [
        [own],
        [([near], first, lambda z: z ^ 1)],
        [([far, cross], inner, lambda z: z ^ 3)],
        [([cross_on, near_on], inner, lambda z: z ^ 2)],
    ]


def work(
    n_dp,
    n_mp,
    img_tokens,
    w_key,
    w_value,
    queries,
    lengths,
    d_out,
    img_pooled,
    w_proj,
    txt_embed,
    inv_temp,
):
    ids = jnp.stack([lax.axis_index("dp"), lax.axis_index("mp")]).astype(jnp.int32)
    captions = queries.shape[0]

    groups = gather_images(img_tokens, n_mp)
    feats = img_pooled.shape[1]

    facts = join_facts(img_pooled, txt_embed)
    mask = 1
    while mask < n_dp:
        got = flip(facts, "dp", n_dp, mask)
        facts, *pooled = append(facts, got, feats if 2 * mask == n_dp else 0)
        mask *= 2

    first = tick(ids)
    parts, turned, others, grads, other_grads = [], [], [], [], []
    for members in groups:
        att, gq, grad, kept, sent = image_group(
            ids, lengths, members, n_dp, w_key, w_value, queries, d_out, first
        )
        parts += [att, gq]
        turned.append(kept)
        others.append(flip(sent, "dp", n_dp, 1))
        grads.append(grad)
        other_grads.append(flip(grad, "dp", n_dp, 1))

    half = n_dp // 2
    early = early_terms(turned[:-1] + others[:-1], grads[:-1] + other_grads[:-1])
    sides = (turned[-1:] + others[-1:], grads[-1:] + other_grads[-1:], early)
    if half == 4:
        dw_key, dw_value = staged_sums(ids, n_dp, sides)
    else:
        dw_key, dw_value = direct_sums(ids, n_dp, sides)
    rules = [m[2] for members in groups for m in members]
    attended, grad_queries = arrange(ids, rules, parts, [len(m) for m in groups])

    (pooled,) = pooled
    pools = [facts] + [flip(pooled, "mp", n_mp, m) for m in range(1, n_mp)]
    terms = similarity_terms(ids, pools, w_proj, captions)
    terms = [terms] + [flip(terms, "mp", n_mp, m) for m in range(1, n_mp)]
    contrast = losses(ids, inv_temp, terms, n_dp, captions)
    return (attended, grad_queries, dw_key, dw_value, contrast)


def solution(mesh):
    placed = (
        P(("dp", "mp"), None, None),
        P(None, "mp"),
        P(None, "mp"),
        P("dp", None, "mp"),
        P("dp"),
        P("dp", None, "mp"),
        P(("dp", "mp"), None),
        P(None, "mp"),
        P("dp", "mp"),
        P(),
    )
    n_dp, n_mp = mesh.shape["dp"], mesh.shape["mp"]
    return jax.shard_map(
        functools.partial(body, n_dp, n_mp),
        mesh=mesh,
        in_specs=placed,
        out_specs=(
            P("dp", None, "mp"),
            P("dp", None, "mp"),
            P("dp", "mp"),
            P("dp", "mp"),
            P(None, "dp"),
        ),
        check_vma=False,
    )
```
